32 devices in a mesh: tensor: 8 (over z, x), expert: 2 (over core), dp: 2 (over y).
Axes of the slice: x: 2, y: 2, z: 4, core: 2. Of those that a mesh axis runs over, the one named last changes fastest.
Arguments:
- tokens: bfloat16 [512, 2048], P(('expert', 'dp')), may hold values from -6 to 6
- tangent: bfloat16 [512, 2048], P(('expert', 'dp')), may hold values from -6 to 6
- cotangent: bfloat16 [512, 2048], P(('expert', 'dp')), may hold values from -0.59765625 to 0.59765625
- expert_ids: int32 [512, 8], P(('expert', 'dp')), may hold values from 0 to 15, all different within a row; in each aligned block of 128 rows (0 to 127, 128 to 255, ...) at most 96 rows name the same one
- gates: float32 [512, 8], P(('expert', 'dp')), may hold values from 0.1 to 1
- w_in: bfloat16 [16, 2, 768, 2048], P(('tensor', 'expert'), None, None, 'dp'), may hold values from -0.125 to 0.125
- v_in: bfloat16 [16, 2, 768, 2048], P(('tensor', 'expert'), None, None, 'dp'), may hold values from -0.125 to 0.125
- w_out: bfloat16 [16, 768, 2048], P(('tensor', 'expert'), None, 'dp'), may hold values from -0.21875 to 0.21875
- v_out: bfloat16 [16, 768, 2048], P(('tensor', 'expert'), None, 'dp'), may hold values from -0.21875 to 0.21875
Outputs:
- hvp_tokens: float32 [512, 2048], P(('expert', 'dp'))
- hvp_in: float32 [16, 2, 768, 2048], P(('tensor', 'expert'), None, None, 'dp')
- hvp_out: float32 [16, 768, 2048], P(('tensor', 'expert'), None, 'dp')
The draws below stay inside these ranges and needn't reach their ends.
Inputs may be any that keep to these rules, and one draw needn't show every extreme that they name: `expert_ids`: each token names 8 different experts; among the tokens of one block of 128 no expert is named more than 96 times, and some expert reaches 96 in some blocks.
All inputs are finite; a program needn't handle non-finite values.
Results may differ from the reference program's by a relative error of at most 0.013.
Values may be sent and summed in bfloat16 or wider, within the bound.
A program may use at most 128 MiB of HBM per device.

```python
import math
import jax
import jax.numpy as jnp
import numpy as np
from jax import lax

D = 2048
FF = 768
TOPK = 8
TOK_DEV = 128
EXPERTS = 16
CAP = 96
TOKENS = 512
N_EXPERT = 2
N_DP = 2


def level_of(rng, extent, pieces, least, high):
    def one(axis_at, blocks):
        draws = jax.random.uniform(jax.random.fold_in(jax.random.fold_in(rng, 6), axis_at), (blocks,), jnp.float32, least / len(pieces), high / len(pieces))
        return jnp.repeat(jnp.exp(draws), extent[axis_at] // blocks).reshape((-1,) + (1,) * (len(extent) - axis_at - 1))

    level = one(*pieces[0])
    for cut in pieces[1:]:
        level = level * one(*cut)
    return level


def routed_block(rng, own, number, rows, number_of, top, reach, slope):
    order = jax.random.permutation(rng, number_of)
    heavy_load, ordinary = shares(number_of, rows * top, reach, slope, True), shares(number_of, rows * top, reach, slope, False)
    places = jnp.arange(number_of)

    def named(tallies, turn):
        used = int((tallies > 0).sum())
        fixed = max(1, used // 4)
        passed = fixed + (places - fixed + turn * (used - fixed)) % max(1, number_of - fixed)
        return jnp.zeros((number_of,), jnp.int32).at[order[jnp.where(places < fixed, places, passed)]].set(jnp.asarray(tallies, jnp.int32))

    tallies = jnp.where(number % 4 == 0, named(heavy_load, number // 4), named(ordinary, number - number // 4 - 1))
    mixed = jax.random.permutation(jax.random.fold_in(own, 3), number_of)
    source_of, receiver = mixed[0:number_of // 2 * 2:2], mixed[1:number_of // 2 * 2:2]
    room = jnp.minimum(tallies[source_of] - 1, reach - tallies[receiver]) // 2
    room = jnp.where((source_of == order[0]) | (receiver == order[0]) | (tallies[receiver] == 0), 0, jnp.maximum(room, 0))
    passed = jax.random.randint(jax.random.fold_in(own, 4), (number_of // 2,), 0, 1 << 20) % (room + 1)
    tallies = tallies.at[source_of].add(-passed).at[receiver].add(passed)
    items = jnp.searchsorted(jnp.cumsum(tallies), jnp.arange(rows * top), side="right").astype(jnp.int32)
    table = items.reshape(top, rows).T
    table = table[jax.random.permutation(jax.random.fold_in(own, 1), rows)]
    turn = jax.random.randint(jax.random.fold_in(own, 2), (rows, 1), 0, top)
    return jnp.take_along_axis(table, (jnp.arange(top)[None, :] + turn) % top, axis=1)


def shares(amount, total, reach, lean, full):
    portions = [(1 << 20) // math.isqrt(standing ** lean) + 1 for standing in range(1, amount + 1)]
    largest = reach if full else min(reach, max(-(-total // amount), total * portions[0] // sum(portions)))
    least = 1 if total - largest >= amount - 1 else 0
    holding, rest = [largest] + [least] * (amount - 1), total - largest - least * (amount - 1)
    while rest > 0:
        free = [i for i in range(1, amount) if holding[i] < largest] or [i for i in range(1, amount) if holding[i] < reach]
        mass, budget = sum([portions[i] for i in free]), rest
        for i in free:
            addition = min(reach - holding[i], max(1, budget * portions[i] // mass), rest)
            holding[i] = holding[i] + addition
            rest = rest - addition
    return np.array(holding)


def scatter_about(rng, extent, width, bound, split=(), kind=jnp.bfloat16):
    factor_of = level_of(rng, extent, split, -0.22, 0.18) if split else 1.0
    entries = jax.random.normal(rng, extent, jnp.float32) * width * factor_of
    return jnp.minimum(jnp.maximum(entries, -bound), bound).astype(kind)


def setup_inputs(seed: int = 0) -> dict:
    key_of = jax.random.split(jax.random.key(seed), 10)
    tokens = scatter_about(key_of[0], (TOKENS, D), 1.0, 6.0, ((0, 4),))
    tangent = scatter_about(key_of[1], (TOKENS, D), 1.0, 6.0, ((0, 4),))
    cotangent = scatter_about(key_of[2], (TOKENS, D), 0.1, 0.59765625, ((0, 4),))
    expert_ids_keys = jax.random.split(jax.random.fold_in(key_of[3], 1), TOKENS // TOK_DEV)
    expert_ids_turns = jax.random.permutation(jax.random.fold_in(key_of[3], 3), TOKENS // TOK_DEV)
    expert_ids = jax.vmap(lambda own, number: routed_block(jax.random.fold_in(key_of[3], 2), own, number, TOK_DEV, EXPERTS, TOPK, CAP, 2))(expert_ids_keys, expert_ids_turns).reshape((TOKENS, TOPK))
    gates = jnp.clip(jnp.exp(math.log(1.0) - 2.3025851 * jax.random.uniform(key_of[4], (TOKENS, TOPK), jnp.float32) ** level_of(key_of[4], (TOKENS, TOPK), ((0, 4),), -0.2, 0.2)), 0.1, 1.0)
    w_in = scatter_about(key_of[5], (EXPERTS, 2, FF, D), D ** -0.5, 0.125, ((0, 16), (3, 2)))
    v_in = scatter_about(key_of[6], (EXPERTS, 2, FF, D), D ** -0.5, 0.125, ((0, 16), (3, 2)))
    w_out = scatter_about(key_of[7], (EXPERTS, FF, D), FF ** -0.5, 0.21875, ((0, 16), (2, 2)))
    v_out = scatter_about(key_of[8], (EXPERTS, FF, D), FF ** -0.5, 0.21875, ((0, 16), (2, 2)))
    return {"tokens": tokens, "tangent": tangent, "cotangent": cotangent, "expert_ids": expert_ids, "gates": gates, "w_in": w_in, "v_in": v_in, "w_out": w_out, "v_out": v_out}


def rounded(value):
    return lax.optimization_barrier(value.astype(jnp.bfloat16)).astype(jnp.float32)


def reference(tokens, tangent, cotangent, expert_ids, gates, w_in, v_in, w_out, v_out):
    blocks = N_EXPERT * N_DP
    pairs = TOK_DEV * TOPK
    picks = expert_ids.reshape(blocks, pairs).astype(jnp.int32)
    onehot = (picks[:, :, None] == jnp.arange(EXPERTS, dtype=jnp.int32)[None, None, :]).astype(jnp.int32)
    running = jnp.cumsum(onehot, axis=1) - 1
    slots = jnp.sum(onehot * running, axis=2).astype(jnp.int32)
    block_ids = jnp.broadcast_to(jnp.arange(blocks, dtype=jnp.int32)[:, None], (blocks, pairs))
    replica = block_ids % N_DP
    source = block_ids // N_DP
    token_ids = block_ids * TOK_DEV + (jnp.arange(pairs, dtype=jnp.int32) // TOPK)[None, :]
    shape = (N_DP, EXPERTS, N_EXPERT, CAP)
    tables = jnp.full(shape, TOKENS, jnp.int32).at[replica, picks, source, slots].set(token_ids)
    scales = jnp.zeros(shape, jnp.float32).at[replica, picks, source, slots].set(gates.reshape(blocks, pairs))
    zero_row = jnp.zeros((1, D), jnp.bfloat16)
    pad_x = jnp.concatenate([tokens, zero_row], axis=0)
    pad_u = jnp.concatenate([tangent, zero_row], axis=0)
    pad_c = jnp.concatenate([cotangent, zero_row], axis=0)

    def one_expert(carry, expert):
        index = tables[:, expert].reshape(N_DP, -1)
        scale = scales[:, expert].reshape(N_DP, -1)
        rows_x = pad_x[index].astype(jnp.float32)
        rows_u = pad_u[index].astype(jnp.float32)
        rows_dy = rounded(scale[:, :, None] * pad_c[index].astype(jnp.float32))
        w_first = w_in[expert].astype(jnp.float32)
        v_first = v_in[expert].astype(jnp.float32)
        w_second = w_out[expert].astype(jnp.float32)
        v_second = v_out[expert].astype(jnp.float32)
        pre = jnp.einsum("prd,gfd->prgf", rows_x, w_first)
        pre_dot = jnp.einsum("prd,gfd->prgf", rows_u, w_first) + jnp.einsum("prd,gfd->prgf", rows_x, v_first)
        gate_pre, up_val = pre[:, :, 0], pre[:, :, 1]
        gate_dot, up_dot = pre_dot[:, :, 0], pre_dot[:, :, 1]
        back = jnp.einsum("prd,fd->prf", rows_dy, w_second)
        back_dot = jnp.einsum("prd,fd->prf", rows_dy, v_second)
        sigma = jax.nn.sigmoid(gate_pre)
        silu_val = gate_pre * sigma
        first = sigma * (1.0 + gate_pre * (1.0 - sigma))
        second = sigma * (1.0 - sigma) * (2.0 + gate_pre * (1.0 - 2.0 * sigma))
        grad_a = back * up_val * first
        grad_b = back * silu_val
        tang_a = back_dot * up_val * first + back * up_dot * first + back * up_val * second * gate_dot
        tang_b = back_dot * silu_val + back * first * gate_dot
        grads = rounded(jnp.stack([grad_a, grad_b], axis=2))
        tangs = rounded(jnp.stack([tang_a, tang_b], axis=2))
        hidden_dot = rounded(first * gate_dot * up_val + silu_val * up_dot)
        partial_value = jnp.einsum("prgf,gfd->prd", tangs, w_first) + jnp.einsum("prgf,gfd->prd", grads, v_first)
        partial_value = rounded(partial_value)
        carry = carry.at[index.reshape(-1)].add(partial_value.reshape(-1, D))
        part_in = jnp.einsum("prd,prgf->pgfd", rows_u, grads) + jnp.einsum("prd,prgf->pgfd", rows_x, tangs)
        part_out = jnp.einsum("prf,prd->pfd", hidden_dot, rows_dy)
        return carry, (jnp.sum(rounded(part_in), axis=0), jnp.sum(rounded(part_out), axis=0))

    start = jnp.zeros((TOKENS + 1, D), jnp.float32)
    total, results = lax.scan(one_expert, start, jnp.arange(EXPERTS, dtype=jnp.int32))
    return total[:TOKENS], results[0], results[1]
```

```python
import jax
import jax.numpy as jnp
from jax import lax
from jax.sharding import PartitionSpec as P


BF = jnp.bfloat16
F32 = jnp.float32


def dot_nt(x, w):
    return lax.dot_general(x, w, (((1,), (1,)), ((), ())), preferred_element_type=F32)


def dot_nn(x, w):
    return lax.dot_general(x, w, (((1,), (0,)), ((), ())), preferred_element_type=F32)


def dot_tn(x, w):
    return lax.dot_general(x, w, (((0,), (0,)), ((), ())), preferred_element_type=F32)


def sum_over(own, axis):
    n = lax.axis_size(axis)
    if n & (n - 1):
        return lax.psum(own.astype(BF), axis).astype(F32)
    step = 1
    while step < n:
        got = lax.ppermute(own.astype(BF), axis, [(i, i ^ step) for i in range(n)])
        own = own + got.astype(F32)
        step *= 2
    return own


def hidden_terms(pre, pre_dot, backs):
    half = pre.shape[1] // 2
    gate_pre, up_val = pre[:, :half], pre[:, half:]
    gate_dot, up_dot = pre_dot[:, :half], pre_dot[:, half:]
    back, back_dot = backs[:, :half], backs[:, half:]
    sigma = jax.nn.sigmoid(gate_pre)
    silu_val = gate_pre * sigma
    first = sigma * (1.0 + gate_pre * (1.0 - sigma))
    second = sigma * (1.0 - sigma) * (2.0 + gate_pre * (1.0 - 2.0 * sigma))
    grad_a = back * up_val * first
    grad_b = back * silu_val
    tang_a = back_dot * up_val * first + back * up_dot * first + back * up_val * second * gate_dot
    tang_b = back_dot * silu_val + back * first * gate_dot
    hidden_dot = first * gate_dot * up_val + silu_val * up_dot
    grads = jnp.concatenate([grad_a, grad_b], axis=1).astype(BF)
    tangs = jnp.concatenate([tang_a, tang_b], axis=1).astype(BF)
    return grads, tangs, hidden_dot.astype(BF)


def shards(tokens, tangent, cotangent, expert_ids, gates, w_in, v_in, w_out, v_out):
    n_tensor = lax.axis_size("tensor")
    n_expert = lax.axis_size("expert")
    n_dp = lax.axis_size("dp")
    rank, core = lax.axis_index("tensor"), lax.axis_index("expert")
    held, _, ff, part = w_in.shape
    all_experts = held * n_tensor * n_expert
    rows, width = tokens.shape
    topk = expert_ids.shape[1]
    cap = min(rows, 3 * rows * topk // (2 * all_experts))

    names = jnp.arange(all_experts, dtype=jnp.int32)
    hit = expert_ids[:, :, None] == names
    table = jnp.where(jnp.any(hit, axis=1), jnp.sum(jnp.where(hit, gates[:, :, None], 0.0), axis=1), -1.0)
    tables = lax.all_gather(table, ("expert", "dp"), axis=0)
    tables = tables.reshape(n_expert, n_dp, rows, all_experts)

    fields = jnp.stack([tokens, tangent, cotangent])
    mine = lax.all_to_all(fields, "dp", split_axis=2, concat_axis=1, tiled=True)
    blocks = [mine.reshape(3, n_dp, rows, part)]
    for shift in range(1, n_expert):
        moved = [((i + shift) % n_expert, i) for i in range(n_expert)]
        blocks.append(lax.ppermute(mine, "expert", moved).reshape(3, n_dp, rows, part))

    low = jnp.tril(jnp.ones((rows, rows), BF))
    weights = [
        (
            w_in[l].reshape(2 * ff, part),
            v_in[l].reshape(2 * ff, part),
            w_out[l],
            v_out[l],
        )
        for l in range(held)
    ]

    def replica(c):
        saved, spread = [], [0.0] * n_expert
        for l in range(held):
            wi, vi, wo, vo = weights[l]
            expert = (rank * n_expert + core) * held + l
            picks, xs, us, ds = [], [], [], []
            for r in range(n_expert):
                gate = tables[lax.rem(core + r, n_expert), c, :, expert]
                on = gate >= 0.0
                slot = dot_nt(on.astype(BF)[None, :], low)[0].astype(jnp.int32) - 1
                pick = (jnp.arange(cap, dtype=jnp.int32)[:, None] == slot[None, :]) & on[None, :]
                scale = jnp.sum(jnp.where(pick, gate[None, :], 0.0), axis=1)
                pick = pick.astype(BF)
                x, u, cot = blocks[r][0, c], blocks[r][1, c], blocks[r][2, c]
                picks.append(pick)
                xs.append(dot_nn(pick, x).astype(BF))
                us.append(dot_nn(pick, u).astype(BF))
                ds.append((scale[:, None] * dot_nn(pick, cot)).astype(BF))
            x, u, dy = (jnp.concatenate(v, axis=0) for v in (xs, us, ds))
            pre = sum_over(dot_nt(x, wi), "dp")
            pre_dot = sum_over(dot_nt(u, wi) + dot_nt(x, vi), "dp")
            backs = sum_over(jnp.concatenate([dot_nt(dy, wo), dot_nt(dy, vo)], axis=1), "dp")
            grads, tangs, hidden = hidden_terms(pre, pre_dot, backs)
            saved.append((x, u, dy, grads, tangs, hidden))
            partial = (dot_nn(tangs, wi) + dot_nn(grads, vi)).astype(BF)
            for r, pick in enumerate(picks):
                spread[r] = spread[r] + dot_tn(pick, partial[r * cap:(r + 1) * cap])
        total = spread[0]
        for r in range(1, n_expert):
            moved = [(i, (i + r) % n_expert) for i in range(n_expert)]
            total = total + lax.ppermute(spread[r].astype(BF), "expert", moved).astype(F32)
        total = total.reshape(n_tensor, rows // n_tensor, part).astype(BF)
        got = lax.all_to_all(total, "tensor", split_axis=0, concat_axis=0, tiled=True)
        return jnp.sum(got.astype(F32), axis=0).astype(BF), saved

    if n_dp <= 2:
        done = [replica(c) for c in range(n_dp)]
        join = lambda *v: jnp.stack(v)
        share, saved = jax.tree.map(join, *done)
    else:
        share, saved = lax.map(replica, jnp.arange(n_dp))

    hvp_in, hvp_out = [], []
    for l in range(held):
        x, u, dy, grads, tangs, hidden = (v.reshape(-1, v.shape[-1]) for v in saved[l])
        both = jnp.concatenate([grads, tangs], axis=0)
        hvp_in.append(dot_tn(both, jnp.concatenate([u, x], axis=0)).reshape(2, ff, part))
        hvp_out.append(dot_tn(hidden, dy))

    share = lax.all_to_all(share, "dp", split_axis=0, concat_axis=2, tiled=True)[0]
    hvp_tokens = lax.all_gather(share, "tensor", axis=0, tiled=True).astype(F32)
    return hvp_tokens, jnp.stack(hvp_in), jnp.stack(hvp_out)


def solution(mesh):
    rows = P(("expert", "dp"), None)
    wide = P(("tensor", "expert"), None, None, "dp")
    tall = P(("tensor", "expert"), None, "dp")
    return jax.shard_map(
        shards,
        mesh=mesh,
        in_specs=(rows, rows, rows, rows, rows, wide, wide, tall, tall),
        out_specs=(rows, wide, tall),
        check_vma=False,
    )
```

```python
import jax
import jax.numpy as jnp
from jax import lax
from jax.sharding import PartitionSpec as P


BF = jnp.bfloat16
F32 = jnp.float32


def dot_nt(x, w):
    return lax.dot_general(x, w, (((1,), (1,)), ((), ())), preferred_element_type=F32)


def dot_nn(x, w):
    return lax.dot_general(x, w, (((1,), (0,)), ((), ())), preferred_element_type=F32)


def dot_tn(x, w):
    return lax.dot_general(x, w, (((0,), (0,)), ((), ())), preferred_element_type=F32)


def sum_over(own, axis):
    n = lax.axis_size(axis)
    if n & (n - 1):
        return lax.psum(own.astype(BF), axis).astype(F32)
    step = 1
    while step < n:
        got = lax.ppermute(own.astype(BF), axis, [(i, i ^ step) for i in range(n)])
        own = own + got.astype(F32)
        step *= 2
    return own


def hidden_terms(pre, pre_dot, backs):
    half = pre.shape[1] // 2
    gate_pre, up_val = pre[:, :half], pre[:, half:]
    gate_dot, up_dot = pre_dot[:, :half], pre_dot[:, half:]
    back, back_dot = backs[:, :half], backs[:, half:]
    sigma = jax.nn.sigmoid(gate_pre)
    silu_val = gate_pre * sigma
    first = sigma * (1.0 + gate_pre * (1.0 - sigma))
    second = sigma * (1.0 - sigma) * (2.0 + gate_pre * (1.0 - 2.0 * sigma))
    grad_a = back * up_val * first
    grad_b = back * silu_val
    tang_a = back_dot * up_val * first + back * up_dot * first + back * up_val * second * gate_dot
    tang_b = back_dot * silu_val + back * first * gate_dot
    hidden_dot = first * gate_dot * up_val + silu_val * up_dot
    grads = jnp.concatenate([grad_a, grad_b], axis=1).astype(BF)
    tangs = jnp.concatenate([tang_a, tang_b], axis=1).astype(BF)
    return grads, tangs, hidden_dot.astype(BF)


def shards(tokens, tangent, cotangent, expert_ids, gates, w_in, v_in, w_out, v_out):
    n_tensor = lax.axis_size("tensor")
    n_expert = lax.axis_size("expert")
    n_dp = lax.axis_size("dp")
    rank, core = lax.axis_index("tensor"), lax.axis_index("expert")
    held, _, ff, part = w_in.shape
    all_experts = held * n_tensor * n_expert
    rows, width = tokens.shape
    topk = expert_ids.shape[1]
    cap = min(rows, 3 * rows * topk // (2 * all_experts))

    around = [
        [((i + r) % n_expert, i) for i in range(n_expert)] for r in range(n_expert)
    ]

    def from_cores(v):
        return [v] + [lax.ppermute(v, "expert", around[r]) for r in range(1, n_expert)]

    fields = (tokens, tangent, cotangent)
    if n_dp == 2:
        low_half = [v[:, :part] for v in fields]
        high_half = [v[:, part:] for v in fields]
        first = lax.axis_index("dp") == 0
        give = jnp.where(first, jnp.concatenate(high_half, axis=1), jnp.concatenate(low_half, axis=1))
        keep = jnp.where(first, jnp.concatenate(low_half, axis=1), jnp.concatenate(high_half, axis=1))
        other = lax.ppermute(give, "dp", [(0, 1), (1, 0)])
        keeps, others = jnp.stack(from_cores(keep)), jnp.stack(from_cores(other))
        blocks = [jnp.where(first, keeps, others), jnp.where(first, others, keeps)]
    else:
        mine = lax.all_to_all(jnp.stack(fields, axis=1), "dp", split_axis=2, concat_axis=0, tiled=True)
        mine = mine.reshape(n_dp, rows, 3 * part)
        blocks = jnp.stack(from_cores(mine), axis=1)

    names = jnp.arange(all_experts, dtype=jnp.int32)
    hit = names[:, None, None] == expert_ids.T[None]
    table = jnp.sum(jnp.where(hit, gates.T[None], 0.0), axis=1)
    table = jnp.where(jnp.any(hit, axis=1), table, -1.0)
    tables = jnp.broadcast_to(table[None], (n_expert * n_dp, all_experts, rows))
    tables = lax.all_to_all(tables, ("expert", "dp"), split_axis=0, concat_axis=0, tiled=True)
    tables = tables.reshape(n_expert, n_dp, all_experts, rows)

    low = jnp.tril(jnp.ones((rows, rows), BF))
    weights = [
        (
            w_in[l].reshape(2 * ff, part),
            v_in[l].reshape(2 * ff, part),
            w_out[l],
            v_out[l],
        )
        for l in range(held)
    ]

    def replica(c):
        saved, spread = [], [0.0] * n_expert
        for l in range(held):
            wi, vi, wo, vo = weights[l]
            expert = (rank * n_expert + core) * held + l
            picks, scales = [], []
            for r in range(n_expert):
                gate = tables[lax.rem(core + r, n_expert), c, expert]
                on = gate >= 0.0
                slot = dot_nt(on.astype(BF)[None, :], low)[0].astype(jnp.int32) - 1
                pick = (jnp.arange(cap, dtype=jnp.int32)[:, None] == slot[None, :]) & on[None, :]
                scales.append(jnp.sum(jnp.where(pick, gate[None, :], 0.0), axis=1))
                picks.append(pick.astype(BF))
            chosen = jnp.einsum(
                "rst,rtd->rsd", jnp.stack(picks), blocks[c], preferred_element_type=F32
            ).reshape(n_expert * cap, 3 * part)
            x = chosen[:, :part].astype(BF)
            u = chosen[:, part:2 * part].astype(BF)
            dy = (jnp.concatenate(scales)[:, None] * chosen[:, 2 * part:]).astype(BF)
            pre = sum_over(dot_nt(x, wi), "dp")
            pre_dot = sum_over(dot_nt(u, wi) + dot_nt(x, vi), "dp")
            backs = sum_over(jnp.concatenate([dot_nt(dy, wo), dot_nt(dy, vo)], axis=1), "dp")
            grads, tangs, hidden = hidden_terms(pre, pre_dot, backs)
            saved.append((x, u, dy, grads, tangs, hidden))
            partial = (dot_nn(tangs, wi) + dot_nn(grads, vi)).astype(BF)
            for r, pick in enumerate(picks):
                spread[r] = spread[r] + dot_tn(pick, partial[r * cap:(r + 1) * cap])
        total = spread[0]
        for r in range(1, n_expert):
            moved = [(i, (i + r) % n_expert) for i in range(n_expert)]
            total = total + lax.ppermute(spread[r].astype(BF), "expert", moved).astype(F32)
        total = total.reshape(n_tensor, rows // n_tensor, part).astype(BF)
        got = lax.all_to_all(total, "tensor", split_axis=0, concat_axis=0, tiled=True)
        return jnp.sum(got.astype(F32), axis=0).astype(BF), saved

    if n_dp <= 2:
        done = [replica(c) for c in range(n_dp)]
        join = lambda *v: jnp.stack(v)
        share, saved = jax.tree.map(join, *done)
    else:
        share, saved = lax.map(replica, jnp.arange(n_dp))

    hvp_in, hvp_out = [], []
    for l in range(held):
        x, u, dy, grads, tangs, hidden = (v.reshape(-1, v.shape[-1]) for v in saved[l])
        both = jnp.concatenate([grads, tangs], axis=0)
        hvp_in.append(dot_tn(both, jnp.concatenate([u, x], axis=0)).reshape(2, ff, part))
        hvp_out.append(dot_tn(hidden, dy))

    share = lax.all_to_all(share, "dp", split_axis=0, concat_axis=2, tiled=True)[0]
    share = jnp.broadcast_to(share[None], (n_tensor,) + share.shape)
    share = lax.all_to_all(share, "tensor", split_axis=0, concat_axis=0, tiled=True)
    hvp_tokens = share.reshape(rows, width).astype(F32)
    return hvp_tokens, jnp.stack(hvp_in), jnp.stack(hvp_out)


def solution(mesh):
    rows = P(("expert", "dp"), None)
    wide = P(("tensor", "expert"), None, None, "dp")
    tall = P(("tensor", "expert"), None, "dp")
    return jax.shard_map(
        shards,
        mesh=mesh,
        in_specs=(rows, rows, rows, rows, rows, wide, wide, tall, tall),
        out_specs=(rows, wide, tall),
        check_vma=False,
    )
```

```python
import jax
import jax.numpy as jnp
from jax import lax
from jax.sharding import PartitionSpec as P


BF = jnp.bfloat16
F32 = jnp.float32


def dot_nt(x, w):
    return lax.dot_general(x, w, (((1,), (1,)), ((), ())), preferred_element_type=F32)


def dot_nn(x, w):
    return lax.dot_general(x, w, (((1,), (0,)), ((), ())), preferred_element_type=F32)


def dot_tn(x, w):
    return lax.dot_general(x, w, (((0,), (0,)), ((), ())), preferred_element_type=F32)


def sum_over(own, axis, sent, ahead=None):
    n = lax.axis_size(axis)
    if n & (n - 1):
        return lax.psum(own.astype(BF), axis).astype(F32)
    step = 1
    while step < n:
        give = own.astype(BF)
        if step == 1:
            sent.append(give)
        got = lax.ppermute(give, axis, [(i, i ^ step) for i in range(n)])
        if ahead is not None:
            got, ahead = lax.optimization_barrier((got, ahead))
        own = own + got.astype(F32)
        step *= 2
    return own


def hidden_terms(pre, pre_dot, backs):
    half = pre.shape[1] // 2
    gate_pre, up_val = pre[:, :half], pre[:, half:]
    gate_dot, up_dot = pre_dot[:, :half], pre_dot[:, half:]
    back, back_dot = backs[:, :half], backs[:, half:]
    sigma = jax.nn.sigmoid(gate_pre)
    silu_val = gate_pre * sigma
    first = sigma * (1.0 + gate_pre * (1.0 - sigma))
    second = sigma * (1.0 - sigma) * (2.0 + gate_pre * (1.0 - 2.0 * sigma))
    grad_a = back * up_val * first
    grad_b = back * silu_val
    tang_a = back_dot * up_val * first + back * up_dot * first + back * up_val * second * gate_dot
    tang_b = back_dot * silu_val + back * first * gate_dot
    hidden_dot = first * gate_dot * up_val + silu_val * up_dot
    grads = jnp.concatenate([grad_a, grad_b], axis=1).astype(BF)
    tangs = jnp.concatenate([tang_a, tang_b], axis=1).astype(BF)
    return grads, tangs, hidden_dot.astype(BF)


def shards(tokens, tangent, cotangent, expert_ids, gates, w_in, v_in, w_out, v_out):
    n_tensor = lax.axis_size("tensor")
    n_expert = lax.axis_size("expert")
    n_dp = lax.axis_size("dp")
    rank, core = lax.axis_index("tensor"), lax.axis_index("expert")
    held, _, ff, part = w_in.shape
    all_experts = held * n_tensor * n_expert
    rows, width = tokens.shape
    topk = expert_ids.shape[1]
    cap = min(rows, 3 * rows * topk // (2 * all_experts))

    around = [
        [((i + r) % n_expert, i) for i in range(n_expert)] for r in range(n_expert)
    ]

    def from_cores(v):
        return [v] + [lax.ppermute(v, "expert", around[r]) for r in range(1, n_expert)]

    fields = (tokens, tangent, cotangent)
    if n_dp == 2:
        low_half = [v[:, :part] for v in fields]
        high_half = [v[:, part:] for v in fields]
        first = lax.axis_index("dp") == 0
        give = jnp.where(first, jnp.concatenate(high_half, axis=1), jnp.concatenate(low_half, axis=1))
        keep = jnp.where(first, jnp.concatenate(low_half, axis=1), jnp.concatenate(high_half, axis=1))
        other = lax.ppermute(give, "dp", [(0, 1), (1, 0)])
        keeps, others = jnp.stack(from_cores(keep)), jnp.stack(from_cores(other))
        blocks = [jnp.where(first, keeps, others), jnp.where(first, others, keeps)]
    else:
        mine = lax.all_to_all(jnp.stack(fields, axis=1), "dp", split_axis=2, concat_axis=0, tiled=True)
        mine = mine.reshape(n_dp, rows, 3 * part)
        blocks = jnp.stack(from_cores(mine), axis=1)

    names = jnp.arange(all_experts, dtype=jnp.int32)
    hit = names[:, None, None] == expert_ids.T[None]
    table = jnp.sum(jnp.where(hit, gates.T[None], 0.0), axis=1)
    table = jnp.where(jnp.any(hit, axis=1), table, -1.0)
    tables = jnp.broadcast_to(table[None], (n_expert * n_dp, all_experts, rows))
    tables = lax.all_to_all(tables, ("expert", "dp"), split_axis=0, concat_axis=0, tiled=True)
    tables = tables.reshape(n_expert, n_dp, all_experts, rows)

    low = jnp.tril(jnp.ones((rows, rows), BF))
    weights = [
        (
            w_in[l].reshape(2 * ff, part),
            v_in[l].reshape(2 * ff, part),
            w_out[l],
            v_out[l],
        )
        for l in range(held)
    ]

    def replica(c, before=None):
        saved, spread, sent = [], [0.0] * n_expert, []
        block, ahead = blocks[c], None
        if before is not None:
            block, _ = lax.optimization_barrier((block, before[2]))
            ahead = before[0]
        for l in range(held):
            wi, vi, wo, vo = weights[l]
            expert = (rank * n_expert + core) * held + l
            picks, scales = [], []
            for r in range(n_expert):
                gate = tables[lax.rem(core + r, n_expert), c, expert]
                on = gate >= 0.0
                slot = dot_nt(on.astype(BF)[None, :], low)[0].astype(jnp.int32) - 1
                pick = (jnp.arange(cap, dtype=jnp.int32)[:, None] == slot[None, :]) & on[None, :]
                scales.append(jnp.sum(jnp.where(pick, gate[None, :], 0.0), axis=1))
                picks.append(pick.astype(BF))
            chosen = jnp.einsum(
                "rst,rtd->rsd", jnp.stack(picks), block, preferred_element_type=F32
            ).reshape(n_expert * cap, 3 * part)
            x = chosen[:, :part].astype(BF)
            u = chosen[:, part:2 * part].astype(BF)
            dy = (jnp.concatenate(scales)[:, None] * chosen[:, 2 * part:]).astype(BF)
            pre = sum_over(dot_nt(x, wi), "dp", sent)
            pre_dot = sum_over(dot_nt(u, wi) + dot_nt(x, vi), "dp", sent)
            backs = sum_over(jnp.concatenate([dot_nt(dy, wo), dot_nt(dy, vo)], axis=1), "dp", sent, ahead)
            grads, tangs, hidden = hidden_terms(pre, pre_dot, backs)
            saved.append((x, u, dy, grads, tangs, hidden))
            partial = (dot_nn(tangs, wi) + dot_nn(grads, vi)).astype(BF)
            for r, pick in enumerate(picks):
                spread[r] = spread[r] + dot_tn(pick, partial[r * cap:(r + 1) * cap])
        total = spread[0]
        for r in range(1, n_expert):
            moved = [(i, (i + r) % n_expert) for i in range(n_expert)]
            total = total + lax.ppermute(spread[r].astype(BF), "expert", moved).astype(F32)
        total = total.reshape(n_tensor, rows // n_tensor, part).astype(BF)
        got = lax.all_to_all(total, "tensor", split_axis=0, concat_axis=0, tiled=True)
        return jnp.sum(got.astype(F32), axis=0).astype(BF), saved, sent

    if n_dp <= 2:
        done = [replica(0)]
        for c in range(1, n_dp):
            done.append(replica(c, done[-1]))
        share, saved = jax.tree.map(lambda *v: jnp.stack(v), *[d[:2] for d in done])
    else:
        share, saved = lax.map(lambda c: replica(c)[:2], jnp.arange(n_dp))

    hvp_in, hvp_out = [], []
    for l in range(held):
        x, u, dy, grads, tangs, hidden = (v.reshape(-1, v.shape[-1]) for v in saved[l])
        both = jnp.concatenate([grads, tangs], axis=0)
        hvp_in.append(dot_tn(both, jnp.concatenate([u, x], axis=0)).reshape(2, ff, part))
        hvp_out.append(dot_tn(hidden, dy))

    share = jnp.broadcast_to(share[None], (n_tensor,) + share.shape)
    share = share.reshape((n_tensor * n_dp,) + share.shape[2:])
    share = lax.all_to_all(share, ("tensor", "dp"), split_axis=0, concat_axis=0, tiled=True)
    share = share.reshape(n_tensor, n_dp, rows // n_tensor, part).transpose(0, 2, 1, 3)
    hvp_tokens = share.reshape(rows, width).astype(F32)
    return hvp_tokens, jnp.stack(hvp_in), jnp.stack(hvp_out)


def solution(mesh):
    rows = P(("expert", "dp"), None)
    wide = P(("tensor", "expert"), None, None, "dp")
    tall = P(("tensor", "expert"), None, "dp")
    return jax.shard_map(
        shards,
        mesh=mesh,
        in_specs=(rows, rows, rows, rows, rows, wide, wide, tall, tall),
        out_specs=(rows, wide, tall),
        check_vma=False,
    )
```
